256 devices in a mesh: dp: 32 (over x, z_hi, core), mp: 8 (over z_lo, y).
Axes of the slice: x: 4, y: 4, z: 8 (z_hi: 4, z_lo: 2; z = z_hi * 2 + z_lo), core: 2. Of those that a mesh axis runs over, the one named last changes fastest.
Arguments:
- tokens: bfloat16 [32, 2048, 2048], P('dp'), may hold values from -80 to 80
- w_query: bfloat16 [2048, 2048], P('dp', 'mp'), may hold values from -0.125 to 0.125
- w_key: bfloat16 [2048, 2048], P('dp', 'mp'), may hold values from -0.125 to 0.125
- w_value: bfloat16 [2048, 2048], P('dp', 'mp'), may hold values from -0.125 to 0.125
- w_out: bfloat16 [2048, 2048], P('mp', 'dp'), may hold values from -0.125 to 0.125
- memory: float32 [16, 128, 128], P('mp', 'dp'), may hold values from -3 to 3
- normalizer: float32 [16, 128], P('mp', 'dp'), may hold values from 0.02 to 0.2
- gate_bias: float32 [16], P('mp'), may hold values from -2 to 2
Outputs:
- output: bfloat16 [32, 2048, 2048], P('dp', None, 'mp')
- memory_new: float32 [16, 128, 128], P('mp', 'dp')
- normalizer_new: float32 [16, 128], P('mp', 'dp')
The draws below stay inside these ranges and needn't reach their ends.
All inputs are finite; a program needn't handle non-finite values.
Results may differ from the reference program's by a relative error of at most 0.025.
Values may be sent and summed in bfloat16 or wider, within the bound.
A program may use at most 128 MiB of HBM per device.

```python
import math
import jax
import jax.numpy as jnp
from jax import lax

D = 2048
H = 16
DH = 128
SEG = 2048
BATCH = 32
N_MP = 8


def draw_tokens(key, part):
    first = jax.random.fold_in(jax.random.fold_in(key, 11), 0)
    values = jax.random.truncated_normal(first, -6.0, 6.0, (BATCH, SEG, D), jnp.float32)
    return values.astype(jnp.bfloat16)


def block_scale(rng, dims, shards, smallest, largest):
    gain, own = 1.0, jax.random.fold_in(rng, 6)
    for position, parts in shards:
        steps = jnp.exp(jax.random.uniform(jax.random.fold_in(own, position), (parts,), jnp.float32, smallest / len(shards), largest / len(shards)))
        gain = gain * jnp.repeat(steps, dims[position] // parts).reshape([-1 if axis == position else 1 for axis in range(len(dims))])
    return gain


def centred(own_key, shape, width, most, pieces=(), held_as=jnp.bfloat16):
    entries = jax.random.normal(own_key, shape, jnp.float32) * width
    if len(pieces) > 0:
        entries = block_scale(own_key, shape, pieces, -0.22, 0.18) * entries
    return jnp.clip(entries, min=-most, max=most).astype(held_as)


def setup_inputs(seed: int = 0) -> dict:
    key_list = jax.random.split(jax.random.key(seed), 9)
    return {
        "tokens": draw_tokens(jax.random.fold_in(key_list[8], 71), 0),
        "w_query": centred(key_list[1], (D, H * DH), D ** -0.5, 0.125, ((0, 32), (1, 8))),
        "w_key": centred(key_list[2], (D, H * DH), D ** -0.5, 0.125, ((0, 32), (1, 8))),
        "w_value": centred(key_list[3], (D, H * DH), D ** -0.5, 0.125, ((0, 32), (1, 8))),
        "w_out": centred(key_list[4], (H * DH, D), (H * DH) ** -0.5, 0.125, ((0, 8), (1, 32))),
        "memory": centred(key_list[5], (H, DH, DH), 0.5, 3.0, ((0, 8), (1, 32)), jnp.float32),
        "normalizer": jnp.clip(jnp.exp(math.log(0.2) - 2.3025851 * jax.random.uniform(key_list[6], (H, DH), jnp.float32) ** block_scale(key_list[6], (H, DH), ((0, 8), (1, 32)), -0.2, 0.2)), 0.02, 0.2),
        "gate_bias": jnp.clip(jax.random.uniform(key_list[7], (H,), jnp.float32, -2.0, 2.0) * block_scale(key_list[7], (H,), ((0, 8),), -0.4, 0.0), -2.0, 2.0),
    }


def feature_map(values):
    return jnp.where(values > 0, values + 1.0, jnp.exp(jnp.minimum(values, 0.0)))

def reference(tokens, w_query, w_key, w_value, w_out, memory, normalizer, gate_bias):
    mixing = jax.nn.sigmoid(gate_bias)
    scale = 1.0 / jnp.sqrt(jnp.float32(DH))
    positions = jnp.arange(SEG)
    allowed = positions[:, None] >= positions[None, :]
    highest = lax.Precision.HIGHEST
    group_heads = H // N_MP

    def one_sequence(sequence):
        shape = (SEG, H, DH)
        query = jnp.dot(sequence, w_query, preferred_element_type=jnp.float32).astype(jnp.bfloat16).reshape(shape)
        keys = jnp.dot(sequence, w_key, preferred_element_type=jnp.float32).astype(jnp.bfloat16).reshape(shape)
        values = jnp.dot(sequence, w_value, preferred_element_type=jnp.float32).astype(jnp.bfloat16).reshape(shape)
        feat_query = feature_map(query.astype(jnp.float32))
        feat_key = feature_map(keys.astype(jnp.float32))
        numer = jnp.einsum('thi,hij->thj', feat_query, memory, precision=highest)
        denom = jnp.einsum('thi,hi->th', feat_query, normalizer, precision=highest)
        retrieved = numer / denom[:, :, None]
        scores = jnp.einsum('thd,shd->hts', query.astype(jnp.float32), keys.astype(jnp.float32)) * scale
        scores = jnp.where(allowed[None], scores, -1e+30)
        probs = jax.nn.softmax(scores, axis=-1).astype(jnp.bfloat16)
        local = jnp.einsum('hts,shd->thd', probs.astype(jnp.float32), values.astype(jnp.float32))
        combined = (mixing[None, :, None] * retrieved + (1.0 - mixing)[None, :, None] * local).astype(jnp.bfloat16)
        grouped = combined.reshape(SEG, N_MP, group_heads * DH).astype(jnp.float32)
        out_groups = w_out.reshape(N_MP, group_heads * DH, D).astype(jnp.float32)
        partials = jnp.einsum('tgc,gcd->gtd', grouped, out_groups).astype(jnp.bfloat16)
        partials = lax.optimization_barrier(partials).astype(jnp.float32)
        output = lax.optimization_barrier(jnp.sum(partials, axis=0)).astype(jnp.bfloat16)
        key_numer = jnp.einsum('thi,hij->thj', feat_key, memory, precision=highest)
        key_denom = jnp.einsum('thi,hi->th', feat_key, normalizer, precision=highest)
        residual = values.astype(jnp.float32) - key_numer / key_denom[:, :, None]
        delta = jnp.einsum('thi,thj->hij', feat_key, residual, precision=highest)
        return (output, delta, lax.optimization_barrier(jnp.sum(feat_key, axis=0)))
    outputs, deltas, key_sums = lax.map(one_sequence, tokens)
    memory_new = memory + lax.optimization_barrier(jnp.sum(deltas, axis=0)) / SEG
    normalizer_new = normalizer + lax.optimization_barrier(jnp.sum(key_sums, axis=0)) / (SEG * BATCH)
    return (outputs, memory_new, normalizer_new)
```

```python
import functools
import math

import jax
import jax.numpy as jnp
from jax import lax
from jax.experimental import pallas as pl
from jax.experimental.pallas import tpu as pltpu
from jax.sharding import PartitionSpec as P

MESH = pl.DeviceIdType.MESH
F32, BF16 = jnp.float32, jnp.bfloat16

NX, NZH, NC = 4, 4, 2
NZL, NY = 2, 4
DP, MP = NX * NZH * NC, NZL * NY
SEG, D, HD, HW = 2048, 2048, 128, 256
SH = D // DP
PW = 4 * HW
CH = 256
NCH = SEG // CH
SCALE2 = math.log2(math.e) / math.sqrt(HD)

ZF, L0, L1 = 144, 80, 208


def nt(a, b):
    return lax.dot_general(a, b, (((1,), (1,)), ((), ())), preferred_element_type=F32)


def nn(a, b):
    return jnp.dot(a, b, preferred_element_type=F32)


def feature(u):
    return jnp.where(u > 0, u + 1.0, jnp.exp(jnp.minimum(u, 0.0)))


def kernel(
    tok_hbm, wsh, memn, memf, normf, gate,
    out, mem_out, norm_out,
    tok, w, wo, keys, vals, gath, qs, scr, mx, acc, mm, memg, dacc, stage, drecv,
    tok_sem, ws_sem, wz_sem, wl_sem, wr_sem, wo_sem, wc_sem,
    ms_sem, mr_sem, as_sem, ar_sem, ab_sem, ds_sem, dr_sem,
    xs_sem, xl_sem, xr_sem, xz_sem, o1_sem, o2_sem, lz_sem, rz_sem, f_sem,
):
    me, mp = lax.axis_index("dp"), lax.axis_index("mp")
    core, zh, x = lax.rem(me, 2), lax.rem(lax.div(me, 2), NZH), lax.div(me, 2 * NZH)
    y, zl = lax.rem(mp, NY), lax.div(mp, NY)

    def dpi(a, b, c):
        return (a * NZH + b) * 2 + c

    def at_dp(d):
        return {"dp": d, "mp": mp}

    def at_mp(m):
        return {"dp": me, "mp": m}

    def send(src, dst, ssem, rsem, dev):
        pltpu.make_async_remote_copy(
            src_ref=src, dst_ref=dst, send_sem=ssem, recv_sem=rsem,
            device_id=dev, device_id_type=MESH,
        ).start()

    def await_bytes(view, sem):
        pltpu.make_async_copy(view, view, sem).wait()

    def token_copy(t):
        rows = pl.ds(pl.multiple_of(t * CH, CH), CH)
        return pltpu.make_async_copy(tok_hbm.at[0, rows], tok.at[rows], tok_sem.at[t])

    for t in range(NCH):
        token_copy(t).start()

    barrier = pltpu.get_barrier_semaphore()
    for k in range(1, DP):
        pl.semaphore_signal(barrier, inc=1, device_id=at_dp(lax.rem(me + k, DP)), device_id_type=MESH)
    for k in range(1, MP):
        pl.semaphore_signal(barrier, inc=1, device_id=at_mp(lax.rem(mp + k, MP)), device_id_type=MESH)

    def shard(d):
        return pl.ds(pl.multiple_of(d * SH, SH), SH)

    def part(d):
        return pl.ds(pl.multiple_of(d * 16, 16), 16)

    w[shard(me), :] = wsh[...]
    memg[part(me), :] = memn[...]
    ones = jnp.ones((SEG, HD), BF16)
    vals[:, HD : 2 * HD] = ones
    vals[:, 3 * HD : 4 * HD] = ones
    dacc[...] = jnp.zeros_like(dacc)
    mm[...] = jnp.zeros_like(mm)
    pl.semaphore_wait(barrier, DP - 1 + MP - 1)

    sib = at_dp(me + 1 - 2 * core)
    xp, xm, xo = lax.rem(x + 1, NX), lax.rem(x + 3, NX), lax.rem(x + 2, NX)
    zr = [zh, lax.rem(zh + 3, NZH), lax.rem(zh + 1, NZH), lax.rem(zh + 2, NZH)]
    right, left = at_dp(dpi(xp, zh, core)), at_dp(dpi(xm, zh, core))

    def hand(src, rows):
        send(src, w.at[rows], ws_sem, wc_sem, sib)

    def spread(src, rows, k):
        send(src, w.at[rows], ws_sem, wl_sem.at[k], right)
        send(src, w.at[rows], ws_sem, wr_sem.at[k], left)

    mine = shard(me)
    spread(wsh, mine, 0)
    for k, z_to in ((1, zr[2]), (2, zr[1]), (3, zr[3])):
        send(wsh, w.at[mine], ws_sem, wz_sem.at[k - 1], at_dp(dpi(x, z_to, core)))
    hand(wsh, mine)
    for k in range(1, DP):
        send(memn, memg.at[part(me)], ms_sem, mr_sem, at_dp(lax.rem(me + k, DP)))

    def from_z(k):
        rows = shard(dpi(x, zr[k], core))
        await_bytes(w.at[rows], wz_sem.at[k - 1])
        spread(w.at[rows], rows, k)
        hand(w.at[rows], rows)

    def from_x(k):
        d = dpi(xm, zr[k], core)
        await_bytes(w.at[shard(d)], wl_sem.at[k])
        half = pl.ds(pl.multiple_of(d * SH, SH), SH // 2)
        send(w.at[half], w.at[half], ws_sem, wo_sem.at[k], right)
        hand(w.at[shard(d)], shard(d))
        d = dpi(xp, zr[k], core)
        await_bytes(w.at[shard(d)], wr_sem.at[k])
        half = pl.ds(pl.multiple_of(d * SH + SH // 2, SH // 2), SH // 2)
        send(w.at[half], w.at[half], ws_sem, wo_sem.at[k], left)
        hand(w.at[shard(d)], shard(d))

    def from_opposite(k):
        rows = shard(dpi(xo, zr[k], core))
        await_bytes(w.at[rows], wo_sem.at[k])
        hand(w.at[rows], rows)

    from_x(0)
    from_z(1)
    from_z(2)
    from_opposite(0)
    from_x(1)
    from_x(2)
    from_z(3)
    from_opposite(1)
    from_opposite(2)
    from_x(3)
    from_opposite(3)
    await_bytes(w.at[pl.ds(0, DP // 2 * SH)], wc_sem)

    half_cols = HW // 2
    mine_half = pl.ds(pl.multiple_of(core * half_cols, half_cols), half_cols)
    for k in range(1, MP):
        m = lax.rem(mp + k, MP)
        rows = pl.ds(pl.multiple_of(m * HW + core * half_cols, half_cols), half_cols)
        send(w.at[rows, pl.ds(3 * HW, HW)], wo.at[mp, mine_half], as_sem, ar_sem, at_mp(m))
    wo[mp] = w[pl.ds(pl.multiple_of(mp * HW, HW), HW), pl.ds(3 * HW, HW)]
    seven_halves = wo.at[pl.ds(0, MP - 1), pl.ds(0, half_cols)]

    await_bytes(memg.at[pl.ds(0, (DP - 1) * 16)], mr_sem)
    r = lax.broadcasted_iota(jnp.int32, (HD, DP * 16), 0)
    c = lax.broadcasted_iota(jnp.int32, (HD, DP * 16), 1)
    base = (r >> 2) * 16 + (r & 3)
    for h in range(2):
        for q in range(2):
            pick = (c == base + (h * 4 + q * 8)).astype(F32).astype(BF16)
            mm[h * HD : (h + 1) * HD, q * HW + h * HD : q * HW + (h + 1) * HD] = nn(
                pick, memg[...]
            ).astype(BF16)

    yp = zl * NY + lax.rem(y + 1, NY)
    ym = zl * NY + lax.rem(y + 3, NY)
    yo = zl * NY + lax.rem(y + 2, NY)
    zz = (1 - zl) * NY + y
    zyp = (1 - zl) * NY + lax.rem(y + 1, NY)
    zym = (1 - zl) * NY + lax.rem(y + 3, NY)
    to_yp, to_ym, to_z = at_mp(yp), at_mp(ym), at_mp(zz)

    def piece(m, t, lo, hi):
        return gath.at[m, pl.ds(pl.multiple_of(t * CH + lo, 16), hi - lo)]

    def compute(t):
        token_copy(t).wait()
        rows = pl.ds(pl.multiple_of(t * CH, CH), CH)
        qkv = nn(tok[rows, :], w[:, pl.ds(0, 3 * HW)])
        q, k, v = (qkv[:, i * HW : (i + 1) * HW].astype(BF16) for i in range(3))
        qs[...] = q
        keys[rows, :] = k
        vals[rows, pl.ds(0, HD)] = v[:, :HD]
        vals[rows, pl.ds(2 * HD, HD)] = v[:, HD:]
        fk = feature(k.astype(F32)).astype(BF16)
        rk = nn(fk, mm[...])
        residual = (v.astype(F32) - rk[:, :HW] / rk[:, HW:]).astype(BF16)
        both = jnp.concatenate([residual, jnp.ones((CH, HD), BF16)], axis=1)
        dacc[...] += lax.dot_general(fk, both, (((0,), (0,)), ((), ())), preferred_element_type=F32)

        mx[...] = jnp.full_like(mx, -jnp.inf)
        acc[...] = jnp.zeros_like(acc)

        def score(j, masked):
            cols = pl.ds(pl.multiple_of(j * CH, CH), CH)
            for h in range(2):
                hs = pl.ds(h * HD, HD)
                s = nt(qs[:, hs], keys[cols, hs])
                if masked:
                    a = lax.broadcasted_iota(jnp.int32, (CH, CH), 0)
                    b = lax.broadcasted_iota(jnp.int32, (CH, CH), 1)
                    s = jnp.where(a >= b, s, -1e37)
                scr[h, :, cols] = s
                mx[h] = jnp.maximum(mx[h], jnp.maximum(s[:, :HD], s[:, HD:]))

        @pl.loop(0, t)
        def _(j):
            score(j, False)

        score(t, True)
        top = [jnp.max(mx[h], axis=1, keepdims=True) for h in range(2)]
        for h in range(2):
            mx[h] = jnp.broadcast_to(top[h], (CH, HD))

        @pl.loop(0, t + 1)
        def _(j):
            cols = pl.ds(pl.multiple_of(j * CH, CH), CH)
            for h in range(2):
                m = jnp.concatenate([mx[h], mx[h]], axis=1)
                p = jnp.exp2((scr[h, :, cols] - m) * SCALE2).astype(BF16)
                acc[h] += nn(p, vals[cols, pl.ds(h * HW, HW)])

        fq = feature(qs[...].astype(F32)).astype(BF16)
        rq = nn(fq, mm[...])
        local = jnp.concatenate([acc[h, :, :HD] / acc[h, :, HD:] for h in range(2)], axis=1)
        g = gate[...]
        gath[mp, rows, :] = (g * (rq[:, :HW] / rq[:, HW:]) + (1.0 - g) * local).astype(BF16)

    def first_sends(t):
        own = piece(mp, t, 0, CH)
        send(own, own, xs_sem.at[t], xl_sem.at[t], to_yp)
        send(own, own, xs_sem.at[t], xr_sem.at[t], to_ym)
        send(own, own, xs_sem.at[t], xz_sem.at[t], to_z)

    def pass_on(m, t, lo, hi, rsem, dev):
        send(piece(m, t, lo, hi), piece(m, t, lo, hi), xs_sem.at[t], rsem.at[t], dev)

    def second_sends(t):
        await_bytes(piece(zz, t, 0, CH), xz_sem.at[t])
        pass_on(zz, t, 0, ZF, lz_sem, to_yp)
        pass_on(zz, t, 0, ZF, rz_sem, to_ym)
        await_bytes(piece(ym, t, 0, CH), xl_sem.at[t])
        pass_on(ym, t, L0, L1, o1_sem, to_yp)
        pass_on(ym, t, ZF, CH, f_sem, to_z)
        await_bytes(piece(yp, t, 0, CH), xr_sem.at[t])
        pass_on(yp, t, 0, L0, o2_sem, to_ym)
        pass_on(yp, t, L1, CH, o2_sem, to_ym)
        pass_on(yp, t, ZF, CH, f_sem, to_z)

    def third_sends(t):
        await_bytes(piece(zym, t, 0, ZF), lz_sem.at[t])
        pass_on(zym, t, L0, ZF, f_sem, to_yp)
        await_bytes(piece(zyp, t, 0, ZF), rz_sem.at[t])
        pass_on(zyp, t, 0, L0, f_sem, to_ym)
        await_bytes(piece(yo, t, L0, L1), o1_sem.at[t])
        pass_on(yo, t, ZF, L1, f_sem, to_z)
        await_bytes(piece(yo, t, 0, CH - L1 + L0), o2_sem.at[t])
        pass_on(yo, t, L1, CH, f_sem, to_z)

    last_rows = 3 * (CH - ZF) + ZF

    def project(t):
        await_bytes(gath.at[0, pl.ds(0, last_rows)], f_sem.at[t])
        rows = pl.ds(pl.multiple_of(t * CH, CH), CH)
        total = nt(gath[0, rows, :], wo[0])
        for m in range(1, MP):
            total += nt(gath[m, rows, :], wo[m])
        out[rows, :] = total.astype(BF16)

    def send_updates():
        d = dacc[...].astype(BF16)
        deltas = jnp.concatenate([d[:HD, :HD], d[HD:, HD : 2 * HD]], axis=0)
        sums = d[:, 2 * HD :]
        r = lax.broadcasted_iota(jnp.int32, (DP * 16, HW), 0)
        c = lax.broadcasted_iota(jnp.int32, (DP * 16, HW), 1)
        hit = c == (r >> 4) * 4 + (r & 3) + ((r >> 2) & 1) * HD
        for src, wanted in ((deltas, 0), (sums, 1)):
            pick = (hit & (((r >> 3) & 1) == wanted)).astype(F32).astype(BF16)
            got = nn(pick, src)
            if wanted == 0:
                first = got
        stage[...] = (first + got).astype(BF16)
        drecv[part(me), :] = stage[part(me), :]
        for k in range(1, DP):
            d_to = lax.rem(me + k, DP)
            send(stage.at[part(d_to)], drecv.at[part(me)], ds_sem, dr_sem, at_dp(d_to))

    @pl.loop(0, NCH + 3)
    def _(t):
        @pl.when(t < NCH)
        def _():
            compute(t)
            first_sends(t)

        @pl.when(t == NCH - 1)
        def _():
            send_updates()

        @pl.when((t >= 1) & (t <= NCH))
        def _():
            second_sends(t - 1)

        @pl.when(t == 1)
        def _():
            await_bytes(seven_halves, ar_sem)
            for k in range(1, MP):
                m = lax.rem(mp + k, MP)
                send(wo.at[m, mine_half], wo.at[m, mine_half], as_sem, ab_sem, sib)

        @pl.when((t >= 2) & (t <= NCH + 1))
        def _():
            third_sends(t - 2)

        @pl.when(t == 3)
        def _():
            await_bytes(seven_halves, ab_sem)

        @pl.when(t >= 3)
        def _():
            project(t - 3)

    await_bytes(drecv.at[pl.ds(0, (DP - 1) * 16)], dr_sem)
    total = jnp.sum(drecv[...].astype(F32).reshape(DP, 16, HD), axis=0)
    mem_out[...] = memf[...] + total[:8] / SEG
    norm_out[...] = normf[...] + total[8:] / (SEG * DP)

    await_bytes(w.at[pl.ds(0, 31 * SH)], ws_sem)
    await_bytes(memg.at[pl.ds(0, (DP - 1) * 16)], ms_sem)
    await_bytes(stage.at[pl.ds(0, (DP - 1) * 16)], ds_sem)
    await_bytes(wo.at[pl.ds(0, MP - 1)], as_sem)
    for t in range(NCH):
        await_bytes(gath.at[pl.ds(0, MP - 1), pl.ds(0, CH)], xs_sem.at[t])


def body(tokens, w_query, w_key, w_value, w_out, memory, normalizer, gate_bias):
    wsh = jnp.concatenate([w_query, w_key, w_value, w_out.T], axis=1)
    memf = memory.reshape(8, HD)
    normf = jnp.broadcast_to(normalizer.reshape(8, 1), (8, HD))
    memn = jnp.concatenate([memf, normf], axis=0).astype(BF16)
    gate = jnp.repeat(jax.nn.sigmoid(gate_bias), HD)[None, :]
    dma, vmem = pltpu.SemaphoreType.DMA, pltpu.VMEM
    in_vmem = pl.BlockSpec(memory_space=vmem)
    out, mem_new, norm_new = pl.pallas_call(
        kernel,
        out_shape=(
            jax.ShapeDtypeStruct((SEG, HW), BF16),
            jax.ShapeDtypeStruct((8, HD), F32),
            jax.ShapeDtypeStruct((8, HD), F32),
        ),
        in_specs=[pl.BlockSpec(memory_space=pl.ANY)] + [in_vmem] * 5,
        out_specs=(in_vmem,) * 3,
        scratch_shapes=[
            vmem((SEG, D), BF16),
            vmem((D, PW), BF16),
            vmem((MP, HW, HW), BF16),
            vmem((SEG, HW), BF16),
            vmem((SEG, 2 * HW), BF16),
            vmem((MP, SEG, HW), BF16),
            vmem((CH, HW), BF16),
            vmem((2, CH, SEG), F32),
            vmem((2, CH, HD), F32),
            vmem((2, CH, HW), F32),
            vmem((HW, 2 * HW), BF16),
            vmem((DP * 16, HD), BF16),
            vmem((HW, 3 * HD), F32),
            vmem((DP * 16, HD), BF16),
            vmem((DP * 16, HD), BF16),
            dma((NCH,)), dma, dma((3,)), dma((4,)), dma((4,)), dma((4,)), dma,
            dma, dma, dma, dma, dma, dma, dma,
        ] + [dma((NCH,))] * 9,
        compiler_params=pltpu.CompilerParams(
            collective_id=0, has_side_effects=True, vmem_limit_bytes=58 * 1024 * 1024
        ),
        name="segment_step",
    )(tokens, wsh, memn, memf, normf, gate)
    return (
        out.reshape(1, SEG, HW),
        mem_new.reshape(2, 4, HD),
        norm_new[:, 0].reshape(2, 4),
    )


def solution(mesh):
    in_specs = (
        P("dp", None, None),
        P("dp", "mp"),
        P("dp", "mp"),
        P("dp", "mp"),
        P("mp", "dp"),
        P("mp", "dp", None),
        P("mp", "dp"),
        P("mp"),
    )
    out_specs = (P("dp", None, "mp"), P("mp", "dp", None), P("mp", "dp"))
    return jax.shard_map(body, mesh=mesh, in_specs=in_specs, out_specs=out_specs, check_vma=False)
```
